32 devices in a mesh: stream: 4 (over y, x), tm: 8 (over z, core).
Axes of the slice: x: 2, y: 2, z: 4, core: 2. Of those that a mesh axis runs over, the one named last changes fastest.
Arguments:
- voltages: float32 [2, 4096, 4096], P(None, ('stream', 'tm')), parts along dimension 1, may hold values from -100 to 100
- taps: float32 [16, 4096], replicated, may hold values from -1.5 to 1.5
- flags: int32 [128], P('stream'), parts along dimension 0, may hold values from 0 to 1, as said below
Outputs:
- dynamic: float32 [1024, 4096], P('stream', 'tm'), parts along dimension 0
- kurtosis: float32 [16384], P(('stream', 'tm')), parts along dimension 0
- spectrum: float32 [16384], P(('stream', 'tm')), parts along dimension 0
The draws below stay inside these ranges and needn't reach their ends.
There are 4 independent parts, one for each index of `stream`. The reference program is written for one: setup_inputs(seed, part) draws one part's arguments, and reference() takes and returns one part's arrays. A program takes and returns all parts, laid end to end along the dimension named above; an argument that names none is the same for every part. Nothing has to cross between parts.
Inputs may be any that keep to these rules, and one draw needn't show every extreme that they name: `flags`: at least one and at most 16 blocks of a stream are flagged.
All inputs are finite; a program needn't handle non-finite values.
Results may differ from the reference program's by a relative error of at most 0.00016.
Values sent between devices are 32-bit elements; how exact they have to be, the bound alone decides.
A program may use at most 64 MiB of HBM per device.

```python
import jax
import jax.numpy as jnp
from jax import lax

CHANNEL_COUNT = 4096
TAPS = 16
FLAG_BLOCK = 128
SUMMED = 4
FRAMES = 1024
BLOCKS = 32


def draw_voltages(key, part):
    full_shape = (2, FRAMES, CHANNEL_COUNT)
    frame_place = jnp.arange(FRAMES, dtype=jnp.float32) / max(FRAMES - 1, 1)
    drift_gain = jnp.sqrt(1.0 + 2.0 * frame_place)[None, :, None]
    rough_part = jax.random.truncated_normal(key, -6.0, 6.0, full_shape, jnp.float32)
    values = rough_part * drift_gain
    return jnp.clip(values, -100.0, 100.0).astype(jnp.float32)


def draw_flags(key, part):
    ranking = jax.random.permutation(key, BLOCKS)
    flagged_count = jax.random.randint(jax.random.fold_in(key, 1), (), 1, BLOCKS // 2 + 1)
    return (ranking < flagged_count).astype(jnp.int32)


def normal_values(rng, extent, deviation, reach, held_as=jnp.bfloat16):
    return jnp.clip(deviation * jax.random.normal(rng, extent, jnp.float32), -reach, reach).astype(held_as)


def setup_inputs(seed: int = 0, part: int = 0) -> dict:
    key_of = jax.random.split(jax.random.key(seed), 4)
    part_splits = jax.random.split(jax.random.fold_in(key_of[3], part), 4)
    voltages = draw_voltages(jax.random.fold_in(jax.random.fold_in(key_of[3], part), 71), part)
    taps = normal_values(key_of[1], (TAPS, CHANNEL_COUNT), TAPS ** -0.5, 1.5, jnp.float32)
    flags = draw_flags(jax.random.fold_in(jax.random.fold_in(key_of[3], part), 71), part)
    return {"voltages": voltages, "taps": taps, "flags": flags}


def reference(voltages, taps, flags):
    frames = voltages.shape[1]
    padded = jnp.pad(voltages, ((0, 0), (TAPS - 1, 0), (0, 0)))
    filtered = jnp.zeros(voltages.shape, jnp.float32)
    for offset in range(TAPS):
        begin = TAPS - 1 - offset
        filtered = filtered + taps[offset][None, None, :] * padded[:, begin:begin + frames, :]
    spectra = jnp.fft.fft(filtered[0] + 1j * filtered[1], axis=-1)
    real_part = jnp.real(spectra)
    imag_part = jnp.imag(spectra)
    channel_powers = real_part * real_part + imag_part * imag_part
    mean_power = jnp.sum(channel_powers, axis=0)
    second_moment = jnp.sum(channel_powers * channel_powers, axis=0)
    kurtosis = ((frames + 1.0) / (frames - 1.0)) * (frames * second_moment / (mean_power * mean_power) - 1.0)
    clean_count = (1 - jnp.repeat(flags, FLAG_BLOCK)).astype(jnp.float32)
    group_sum = jnp.sum(channel_powers * clean_count[None, :])
    spectrum = CHANNEL_COUNT * clean_count * mean_power / group_sum
    integrated_power = jnp.sum(channel_powers.reshape(frames // SUMMED, SUMMED, CHANNEL_COUNT), axis=1)
    row_sum = jnp.dot(integrated_power, clean_count, precision=lax.Precision.HIGHEST)
    dynamic = CHANNEL_COUNT * clean_count[None, :] * integrated_power / row_sum[:, None]
    return dynamic, kurtosis, spectrum
```

```python
import functools
import math

import jax
import jax.numpy as jnp
import numpy as np
from jax import lax
from jax.experimental import pallas as pl
from jax.experimental.pallas import tpu as pltpu
from jax.sharding import PartitionSpec as P

SUMMED = 4
LANES = 128
ROWS = 8


def rotate_by(value, k, n):
    re, im = value
    if k == 0:
        return re, im
    if 4 * k == n:
        return im, -re
    half = math.sqrt(0.5)
    if 8 * k == n:
        return (re + im) * half, (im - re) * half
    if 8 * k == 3 * n:
        return (im - re) * half, (re + im) * (-half)
    c = math.cos(2.0 * math.pi * k / n)
    s = math.sin(2.0 * math.pi * k / n)
    return re * c + im * s, im * c - re * s


def fft(values):
    n = len(values)
    if n == 1:
        return values
    even = fft(values[0::2])
    odd = fft(values[1::2])
    low, high = [], []
    for k in range(n // 2):
        tr, ti = rotate_by(odd[k], k, n)
        er, ei = even[k]
        low.append((er + tr, ei + ti))
        high.append((er - tr, ei - ti))
    return low + high


def kernel(n, x_hbm, taps_ref, flags_ref, cos_ref, sin_ref, wa_ref, wb_ref,
           dyn_hbm, kurt_ref, spec_ref,
           xbuf, ybuf, zbuf, m1buf, m2buf, bbuf, tbuf, vbuf, sendbuf, recvbuf,
           load_sem, halo_send, halo_recv, send_sem, recv_sem, out_sem):
    me = lax.axis_index("tm")
    frames, channels = x_hbm.shape[1], x_hbm.shape[2]
    tap_count = taps_ref.shape[0]
    head = xbuf.shape[2] - frames
    outer = channels // LANES
    span = LANES // outer
    step = SUMMED * ROWS
    chunks = frames // step
    part = channels // n
    blocks = flags_ref.shape[0]
    width = channels // blocks

    def load(i, a):
        return pltpu.make_async_copy(
            x_hbm.at[:, pl.ds(i * step, step), pl.ds(pl.multiple_of(a * LANES, LANES), LANES)],
            xbuf.at[:, a, pl.ds(head + i * step, step), :], load_sem.at[i])

    def loaded(i):
        rows = xbuf.at[:, :, pl.ds(head + i * step, step), :]
        pltpu.make_async_copy(rows, rows, load_sem.at[i]).wait()

    for i in range(chunks):
        def start_load(a, carry, i=i):
            load(i, a).start()
            return carry

        lax.fori_loop(0, outer, start_load, 0)

    barrier = pltpu.get_barrier_semaphore()

    def greet(off, carry):
        pl.semaphore_signal(barrier, inc=1, device_id={"tm": lax.rem(me + off, n)},
                            device_id_type=pl.DeviceIdType.MESH)
        return carry

    lax.fori_loop(1, n, greet, 0)
    pl.semaphore_wait(barrier, n - 1)

    def halo(a):
        return pltpu.make_async_remote_copy(
            src_ref=x_hbm.at[:, pl.ds(frames - head, head), pl.ds(pl.multiple_of(a * LANES, LANES), LANES)],
            dst_ref=xbuf.at[:, a, pl.ds(0, head), :],
            send_sem=halo_send, recv_sem=halo_recv,
            device_id={"tm": lax.rem(me + 1, n)}, device_id_type=pl.DeviceIdType.MESH)

    def whole_halo():
        return pltpu.make_async_remote_copy(
            src_ref=xbuf.at[:, :, pl.ds(0, head), :],
            dst_ref=xbuf.at[:, :, pl.ds(0, head), :],
            send_sem=halo_send, recv_sem=halo_recv,
            device_id={"tm": lax.rem(me + 1, n)}, device_id_type=pl.DeviceIdType.MESH)

    @pl.when(me < n - 1)
    def _():
        def start_halo(a, carry):
            halo(a).start()
            return carry

        lax.fori_loop(0, outer, start_halo, 0)

    @pl.when(me == 0)
    def _():
        xbuf[:, :, 0:head, :] = jnp.zeros((2, outer, head, LANES), jnp.float32)

    m1buf[...] = jnp.zeros_like(m1buf)
    m2buf[...] = jnp.zeros_like(m2buf)
    lane = lax.broadcasted_iota(jnp.int32, (1, LANES), 1)
    clean = []
    clean_row = jnp.zeros((1, LANES), jnp.float32)
    for b in range(blocks):
        clean.append((1 - flags_ref[b]).astype(jnp.float32))
        clean_row = jnp.where(lane // (width // outer) == b, clean[b], clean_row)

    def relayout(count):
        for g in range(-(-count * outer // LANES)):
            tbuf[g] = bbuf[g * LANES:(g + 1) * LANES, :].T
        for r in range(count):
            g, place = (r * outer) // LANES, (r * outer) % LANES
            total = None
            for e1 in range(span):
                piece = tbuf[g, pl.ds(e1, outer, stride=span), :]
                shift = (e1 * outer - place) % LANES
                if shift:
                    piece = pltpu.roll(piece, shift, 1)
                total = piece if total is None else jnp.where(lane // outer == e1, piece, total)
            vbuf[r * outer:(r + 1) * outer, :] = total

    def send(first, count, slot, off):
        other = lax.rem(me + off, n)
        return pltpu.make_async_remote_copy(
            src_ref=sendbuf.at[pl.ds(first, count), pl.ds(pl.multiple_of(other * part, LANES), part)],
            dst_ref=recvbuf.at[me, pl.ds(first, count), :],
            send_sem=send_sem.at[slot, off], recv_sem=recv_sem.at[slot, me],
            device_id={"tm": other}, device_id_type=pl.DeviceIdType.MESH)

    def arrival(first, count, slot, source):
        return pltpu.make_async_remote_copy(
            src_ref=sendbuf.at[pl.ds(first, count), pl.ds(0, part)],
            dst_ref=recvbuf.at[source, pl.ds(first, count), :],
            send_sem=send_sem.at[slot, 0], recv_sem=recv_sem.at[slot, source],
            device_id={"tm": source}, device_id_type=pl.DeviceIdType.MESH)

    pieces = []
    order = list(range(1, chunks)) + [0]
    for slot, chunk in enumerate(order):
        if slot == 0:
            loaded(0)
        if chunk:
            loaded(chunk)
        else:
            @pl.when(me > 0)
            def _():
                whole_halo().wait_recv()
        base = head + chunk * step

        def fir(a, carry):
            columns = pl.ds(pl.multiple_of(a * LANES, LANES), LANES)
            coefficients = [jnp.broadcast_to(taps_ref[pl.ds(k, 1), columns], (ROWS, LANES))
                            for k in range(tap_count)]
            for s in range(2):
                sums = [None] * SUMMED
                for o in range(1 - tap_count, SUMMED):
                    value = xbuf[s, a, pl.ds(base + o, ROWS, stride=SUMMED), :]
                    for j in range(SUMMED):
                        if 0 <= j - o < tap_count:
                            term = coefficients[j - o] * value
                            sums[j] = term if sums[j] is None else sums[j] + term
                for j in range(SUMMED):
                    ybuf[s, a, j * ROWS:(j + 1) * ROWS, :] = sums[j]
            return carry

        lax.fori_loop(0, outer, fir, 0)

        def columns_fft(j, carry):
            rows = pl.ds(pl.multiple_of(j * ROWS, ROWS), ROWS)
            result = fft([(ybuf[0, a, rows, :], ybuf[1, a, rows, :]) for a in range(outer)])
            for d in range(outer):
                re, im = result[d]
                c, s = cos_ref[d:d + 1, :], sin_ref[d:d + 1, :]
                zbuf[d, rows, 0:LANES] = re * c + im * s
                zbuf[d, rows, LANES:2 * LANES] = im * c - re * s
            return carry

        lax.fori_loop(0, SUMMED, columns_fft, 0)

        group = 8

        def lanes_dft(g, row_sum):
            z = zbuf[pl.ds(g * group, group), :, :].reshape(group * step, 2 * LANES)
            high = z.astype(jnp.bfloat16)
            low = (z - high.astype(jnp.float32)).astype(jnp.bfloat16)
            y = (jnp.dot(high, wa_ref[...], preferred_element_type=jnp.float32)
                 + jnp.dot(low, wa_ref[...], preferred_element_type=jnp.float32)
                 + jnp.dot(high, wb_ref[...], preferred_element_type=jnp.float32))
            re, im = y[:, :LANES], y[:, LANES:]
            power = re * re + im * im
            for k in range(group):
                piece = [power[k * step + j * ROWS:k * step + (j + 1) * ROWS] for j in range(SUMMED)]
                first = (piece[0] + piece[1]) + (piece[2] + piece[3])
                second = ((piece[0] * piece[0] + piece[1] * piece[1])
                          + (piece[2] * piece[2] + piece[3] * piece[3]))
                d = g * group + k
                bbuf[pl.ds(d, ROWS, stride=outer), :] = first
                m1buf[d] = m1buf[d] + first
                m2buf[d] = m2buf[d] + second
                row_sum = row_sum + first
            return row_sum

        row_sum = lax.fori_loop(0, outer // group, lanes_dft, jnp.zeros((ROWS, LANES), jnp.float32))
        row_total = jnp.sum(row_sum * clean_row, axis=1, keepdims=True)
        scale = channels / row_total
        relayout(ROWS)
        first_row = ROWS * (1 + chunk)
        for q in range(outer):
            tile = vbuf[pl.ds(q, ROWS, stride=outer), :]
            sendbuf[first_row:first_row + ROWS, q * LANES:(q + 1) * LANES] = (
                tile * (scale * clean[q * LANES // width]))
        count = ROWS
        if slot == chunks - 1:
            first = jnp.sum(m1buf[...], axis=1)
            second = jnp.sum(m2buf[...], axis=1)
            bbuf[0:outer, :] = first
            bbuf[outer:2 * outer, :] = second
            bbuf[2 * outer:, :] = jnp.zeros((bbuf.shape[0] - 2 * outer, LANES), jnp.float32)
            relayout(2)
            group_sum = jnp.sum(jnp.sum(first, axis=0, keepdims=True) * clean_row, axis=1, keepdims=True)
            vbuf[2 * outer:3 * outer, :] = jnp.broadcast_to(group_sum, (outer, LANES))
            for q in range(outer):
                sendbuf[0:ROWS, q * LANES:(q + 1) * LANES] = vbuf[pl.ds(q, ROWS, stride=outer), :]
            first_row, count = 0, 2 * ROWS
        pieces.append((first_row, count))

        def start(off, carry, first_row=first_row, count=count, slot=slot):
            send(first_row, count, slot, off).start()
            return carry

        lax.fori_loop(1, n, start, 0)
        recvbuf[me, first_row:first_row + count, :] = sendbuf[
            first_row:first_row + count, pl.ds(pl.multiple_of(me * part, LANES), part)]

    for slot, (first_row, count) in enumerate(pieces):
        def receive(off, carry, first_row=first_row, count=count, slot=slot):
            arrival(first_row, count, slot, lax.rem(me + n - off, n)).wait_recv()
            return carry

        lax.fori_loop(1, n, receive, 0)

    out = pltpu.make_async_copy(recvbuf.at[:, pl.ds(ROWS, chunks * ROWS), :], dyn_hbm, out_sem)
    out.start()
    total = recvbuf[0, 0:ROWS, :]
    for source in range(1, n):
        total = total + recvbuf[source, 0:ROWS, :]
    mean_power, second_moment, whole = total[0:1], total[1:2], total[2:3]
    count = float(frames * n)
    kurt_ref[...] = ((count + 1.0) / (count - 1.0)
                     * (count * second_moment / (mean_power * mean_power) - 1.0))
    own = jnp.zeros((1, part), jnp.float32)
    place = lax.broadcasted_iota(jnp.int32, (1, part), 1) + me * part
    for b in range(blocks):
        own = jnp.where(place // width == b, clean[b], own)
    spec_ref[...] = channels * own * mean_power / whole

    for slot, (first_row, count) in enumerate(pieces):
        def sent(off, carry, first_row=first_row, count=count, slot=slot):
            send(first_row, count, slot, off).wait_send()
            return carry

        lax.fori_loop(1, n, sent, 0)

    @pl.when(me < n - 1)
    def _():
        whole_halo().wait_send()

    out.wait()


def body(n, voltages, taps, flags):
    frames, channels = voltages.shape[1], voltages.shape[2]
    head = -(-(taps.shape[0] - 1) // ROWS) * ROWS
    outer = channels // LANES
    step = SUMMED * ROWS
    chunks = frames // step
    part = channels // n
    turn = 2.0 * np.pi * np.outer(np.arange(outer), np.arange(LANES)) / channels
    angle = 2.0 * np.pi * (np.outer(np.arange(LANES), np.arange(LANES)) % LANES) / LANES
    table = np.block([[np.cos(angle), -np.sin(angle)], [np.sin(angle), np.cos(angle)]]).astype(np.float32)
    table_high = table.astype(jnp.bfloat16)
    table_low = (table - table_high.astype(np.float32)).astype(jnp.bfloat16)
    vmem = pl.BlockSpec(memory_space=pltpu.VMEM)
    dynamic, kurtosis, spectrum = pl.pallas_call(
        functools.partial(kernel, n),
        out_shape=(
            jax.ShapeDtypeStruct((n, chunks * ROWS, part), jnp.float32),
            jax.ShapeDtypeStruct((1, part), jnp.float32),
            jax.ShapeDtypeStruct((1, part), jnp.float32),
        ),
        in_specs=[pl.BlockSpec(memory_space=pl.ANY), vmem, pl.BlockSpec(memory_space=pltpu.SMEM),
                  vmem, vmem, vmem, vmem],
        out_specs=(pl.BlockSpec(memory_space=pl.ANY), vmem, vmem),
        scratch_shapes=[
            pltpu.VMEM((2, outer, head + frames, LANES), jnp.float32),
            pltpu.VMEM((2, outer, step, LANES), jnp.float32),
            pltpu.VMEM((outer, step, 2 * LANES), jnp.float32),
            pltpu.VMEM((outer, ROWS, LANES), jnp.float32),
            pltpu.VMEM((outer, ROWS, LANES), jnp.float32),
            pltpu.VMEM((ROWS * outer, LANES), jnp.float32),
            pltpu.VMEM((ROWS * outer // LANES, LANES, LANES), jnp.float32),
            pltpu.VMEM((ROWS * outer, LANES), jnp.float32),
            pltpu.VMEM(((1 + chunks) * ROWS, channels), jnp.float32),
            pltpu.VMEM((n, (1 + chunks) * ROWS, part), jnp.float32),
            pltpu.SemaphoreType.DMA((chunks,)),
            pltpu.SemaphoreType.DMA,
            pltpu.SemaphoreType.DMA,
            pltpu.SemaphoreType.DMA((chunks, n)),
            pltpu.SemaphoreType.DMA((chunks, n)),
            pltpu.SemaphoreType.DMA,
        ],
        compiler_params=pltpu.CompilerParams(
            collective_id=0, has_side_effects=True, vmem_limit_bytes=40 * 1024 * 1024),
    )(voltages, taps, flags, jnp.asarray(np.cos(turn), jnp.float32), jnp.asarray(np.sin(turn), jnp.float32),
      jnp.asarray(table_high), jnp.asarray(table_low))
    return dynamic.reshape(n * chunks * ROWS, part), kurtosis.reshape(part), spectrum.reshape(part)


def solution(mesh):
    return jax.shard_map(
        functools.partial(body, mesh.shape["tm"]),
        mesh=mesh,
        in_specs=(P(None, ("stream", "tm"), None), P(), P("stream")),
        out_specs=(P("stream", "tm"), P(("stream", "tm")), P(("stream", "tm"))),
        check_vma=False,
    )
```

```python
import functools
import math

import jax
import jax.numpy as jnp
import numpy as np
from jax import lax
from jax.experimental import pallas as pl
from jax.experimental.pallas import tpu as pltpu
from jax.sharding import PartitionSpec as P

SUMMED = 4
LANES = 128
ROWS = 8


def rotate_by(value, k, n):
    re, im = value
    if k == 0:
        return re, im
    if 4 * k == n:
        return im, -re
    half = math.sqrt(0.5)
    if 8 * k == n:
        return (re + im) * half, (im - re) * half
    if 8 * k == 3 * n:
        return (im - re) * half, (re + im) * (-half)
    c = math.cos(2.0 * math.pi * k / n)
    s = math.sin(2.0 * math.pi * k / n)
    return re * c + im * s, im * c - re * s


def fft(values):
    n = len(values)
    if n == 1:
        return values
    even = fft(values[0::2])
    odd = fft(values[1::2])
    low, high = [], []
    for k in range(n // 2):
        tr, ti = rotate_by(odd[k], k, n)
        er, ei = even[k]
        low.append((er + tr, ei + ti))
        high.append((er - tr, ei - ti))
    return low + high


def kernel(n, x_hbm, taps_hbm, flags_hbm, turn_hbm, table_hbm,
           dyn_hbm, kurt_ref, spec_ref,
           taps_ref, flags_ref, turn_ref, table_ref, side_sem, xbuf, ybuf, zbuf, m1buf, m2buf, bbuf, tbuf, vbuf, sendbuf, recvbuf,
           load_sem, halo_send, halo_recv, send_sem, recv_sem, out_sem):
    me = lax.axis_index("tm")
    frames, channels = x_hbm.shape[1], x_hbm.shape[2]
    tap_count = taps_ref.shape[0]
    head = xbuf.shape[2] - frames
    outer = channels // LANES
    span = LANES // outer
    step = SUMMED * ROWS
    chunks = frames // step
    part = channels // n
    blocks = flags_ref.shape[0]
    width = channels // blocks

    def load(i, a):
        return pltpu.make_async_copy(
            x_hbm.at[:, pl.ds(i * step, step), pl.ds(pl.multiple_of(a * LANES, LANES), LANES)],
            xbuf.at[:, a, pl.ds(head + i * step, step), :], load_sem.at[i])

    def loaded(i):
        rows = xbuf.at[:, :, pl.ds(head + i * step, step), :]
        pltpu.make_async_copy(rows, rows, load_sem.at[i]).wait()

    sides = [pltpu.make_async_copy(source, target, side_sem.at[i]) for i, (source, target) in enumerate(
        ((taps_hbm, taps_ref), (flags_hbm, flags_ref), (turn_hbm, turn_ref), (table_hbm, table_ref)))]
    for side in sides:
        side.start()
    for i in range(chunks):
        def start_load(a, carry, i=i):
            load(i, a).start()
            return carry

        lax.fori_loop(0, outer, start_load, 0)

    barrier = pltpu.get_barrier_semaphore()

    def greet(off, carry):
        pl.semaphore_signal(barrier, inc=1, device_id={"tm": lax.rem(me + off, n)},
                            device_id_type=pl.DeviceIdType.MESH)
        return carry

    lax.fori_loop(1, n, greet, 0)
    pl.semaphore_wait(barrier, n - 1)

    def halo(a):
        return pltpu.make_async_remote_copy(
            src_ref=x_hbm.at[:, pl.ds(frames - head, head), pl.ds(pl.multiple_of(a * LANES, LANES), LANES)],
            dst_ref=xbuf.at[:, a, pl.ds(0, head), :],
            send_sem=halo_send, recv_sem=halo_recv,
            device_id={"tm": lax.rem(me + 1, n)}, device_id_type=pl.DeviceIdType.MESH)

    def whole_halo():
        return pltpu.make_async_remote_copy(
            src_ref=xbuf.at[:, :, pl.ds(0, head), :],
            dst_ref=xbuf.at[:, :, pl.ds(0, head), :],
            send_sem=halo_send, recv_sem=halo_recv,
            device_id={"tm": lax.rem(me + 1, n)}, device_id_type=pl.DeviceIdType.MESH)

    @pl.when(me < n - 1)
    def _():
        def start_halo(a, carry):
            halo(a).start()
            return carry

        lax.fori_loop(0, outer, start_halo, 0)

    @pl.when(me == 0)
    def _():
        xbuf[:, :, 0:head, :] = jnp.zeros((2, outer, head, LANES), jnp.float32)

    for side in sides:
        side.wait()
    m1buf[...] = jnp.zeros_like(m1buf)
    m2buf[...] = jnp.zeros_like(m2buf)
    lane = lax.broadcasted_iota(jnp.int32, (1, LANES), 1)
    clean = []
    clean_row = jnp.zeros((1, LANES), jnp.float32)
    for b in range(blocks):
        clean.append((1 - flags_ref[b]).astype(jnp.float32))
        clean_row = jnp.where(lane // (width // outer) == b, clean[b], clean_row)

    def relayout(count):
        for g in range(-(-count * outer // LANES)):
            tbuf[g] = bbuf[g * LANES:(g + 1) * LANES, :].T
        for r in range(count):
            g, place = (r * outer) // LANES, (r * outer) % LANES
            total = None
            for e1 in range(span):
                piece = tbuf[g, pl.ds(e1, outer, stride=span), :]
                shift = (e1 * outer - place) % LANES
                if shift:
                    piece = pltpu.roll(piece, shift, 1)
                total = piece if total is None else jnp.where(lane // outer == e1, piece, total)
            vbuf[r * outer:(r + 1) * outer, :] = total

    def send(first, count, slot, off):
        other = lax.rem(me + off, n)
        return pltpu.make_async_remote_copy(
            src_ref=sendbuf.at[pl.ds(first, count), pl.ds(pl.multiple_of(other * part, LANES), part)],
            dst_ref=recvbuf.at[me, pl.ds(first, count), :],
            send_sem=send_sem.at[slot, off], recv_sem=recv_sem.at[slot, me],
            device_id={"tm": other}, device_id_type=pl.DeviceIdType.MESH)

    def arrival(first, count, slot, source):
        return pltpu.make_async_remote_copy(
            src_ref=sendbuf.at[pl.ds(first, count), pl.ds(0, part)],
            dst_ref=recvbuf.at[source, pl.ds(first, count), :],
            send_sem=send_sem.at[slot, 0], recv_sem=recv_sem.at[slot, source],
            device_id={"tm": source}, device_id_type=pl.DeviceIdType.MESH)

    pieces = []
    order = list(range(1, chunks)) + [0]
    for slot, chunk in enumerate(order):
        if slot == 0:
            loaded(0)
        if chunk:
            loaded(chunk)
        else:
            @pl.when(me > 0)
            def _():
                whole_halo().wait_recv()
        base = head + chunk * step

        def fir(a, carry):
            columns = pl.ds(pl.multiple_of(a * LANES, LANES), LANES)
            coefficients = [jnp.broadcast_to(taps_ref[pl.ds(k, 1), columns], (ROWS, LANES))
                            for k in range(tap_count)]
            for s in range(2):
                sums = [None] * SUMMED
                for o in range(1 - tap_count, SUMMED):
                    value = xbuf[s, a, pl.ds(base + o, ROWS, stride=SUMMED), :]
                    for j in range(SUMMED):
                        if 0 <= j - o < tap_count:
                            term = coefficients[j - o] * value
                            sums[j] = term if sums[j] is None else sums[j] + term
                for j in range(SUMMED):
                    ybuf[s, a, j * ROWS:(j + 1) * ROWS, :] = sums[j]
            return carry

        lax.fori_loop(0, outer, fir, 0, unroll=2)

        def columns_fft(j, carry):
            rows = pl.ds(pl.multiple_of(j * ROWS, ROWS), ROWS)
            result = fft([(ybuf[0, a, rows, :], ybuf[1, a, rows, :]) for a in range(outer)])
            for d in range(outer):
                re, im = result[d]
                c, s = turn_ref[0, d:d + 1, :], turn_ref[1, d:d + 1, :]
                zbuf[d, rows, 0:LANES] = re * c + im * s
                zbuf[d, rows, LANES:2 * LANES] = im * c - re * s
            return carry

        lax.fori_loop(0, SUMMED, columns_fft, 0)

        group = 8

        def lanes_dft(g, row_sum):
            z = zbuf[pl.ds(g * group, group), :, :].reshape(group * step, 2 * LANES)
            high = z.astype(jnp.bfloat16)
            low = (z - high.astype(jnp.float32)).astype(jnp.bfloat16)
            y = (jnp.dot(high, table_ref[0], preferred_element_type=jnp.float32)
                 + jnp.dot(low, table_ref[0], preferred_element_type=jnp.float32)
                 + jnp.dot(high, table_ref[1], preferred_element_type=jnp.float32))
            re, im = y[:, :LANES], y[:, LANES:]
            power = re * re + im * im
            for k in range(group):
                piece = [power[k * step + j * ROWS:k * step + (j + 1) * ROWS] for j in range(SUMMED)]
                first = (piece[0] + piece[1]) + (piece[2] + piece[3])
                second = ((piece[0] * piece[0] + piece[1] * piece[1])
                          + (piece[2] * piece[2] + piece[3] * piece[3]))
                d = g * group + k
                bbuf[pl.ds(d, ROWS, stride=outer), :] = first
                m1buf[d] = m1buf[d] + first
                m2buf[d] = m2buf[d] + second
                row_sum = row_sum + first
            return row_sum

        row_sum = lax.fori_loop(0, outer // group, lanes_dft, jnp.zeros((ROWS, LANES), jnp.float32))
        row_total = jnp.sum(row_sum * clean_row, axis=1, keepdims=True)
        scale = channels / row_total
        relayout(ROWS)
        first_row = ROWS * (1 + chunk)
        for q in range(outer):
            tile = vbuf[pl.ds(q, ROWS, stride=outer), :]
            sendbuf[first_row:first_row + ROWS, q * LANES:(q + 1) * LANES] = (
                tile * (scale * clean[q * LANES // width]))
        count = ROWS
        if slot == chunks - 1:
            first = jnp.sum(m1buf[...], axis=1)
            second = jnp.sum(m2buf[...], axis=1)
            bbuf[0:outer, :] = first
            bbuf[outer:2 * outer, :] = second
            bbuf[2 * outer:, :] = jnp.zeros((bbuf.shape[0] - 2 * outer, LANES), jnp.float32)
            relayout(2)
            group_sum = jnp.sum(jnp.sum(first, axis=0, keepdims=True) * clean_row, axis=1, keepdims=True)
            vbuf[2 * outer:3 * outer, :] = jnp.broadcast_to(group_sum, (outer, LANES))
            for q in range(outer):
                sendbuf[0:ROWS, q * LANES:(q + 1) * LANES] = vbuf[pl.ds(q, ROWS, stride=outer), :]
            first_row, count = 0, 2 * ROWS
        pieces.append((first_row, count))

        def start(off, carry, first_row=first_row, count=count, slot=slot):
            send(first_row, count, slot, off).start()
            return carry

        lax.fori_loop(1, n, start, 0)
        recvbuf[me, first_row:first_row + count, :] = sendbuf[
            first_row:first_row + count, pl.ds(pl.multiple_of(me * part, LANES), part)]

    for slot, (first_row, count) in enumerate(pieces):
        def receive(off, carry, first_row=first_row, count=count, slot=slot):
            arrival(first_row, count, slot, lax.rem(me + n - off, n)).wait_recv()
            return carry

        lax.fori_loop(1, n, receive, 0)

    out = pltpu.make_async_copy(recvbuf.at[:, pl.ds(ROWS, chunks * ROWS), :], dyn_hbm, out_sem)
    out.start()
    total = recvbuf[0, 0:ROWS, :]
    for source in range(1, n):
        total = total + recvbuf[source, 0:ROWS, :]
    mean_power, second_moment, whole = total[0:1], total[1:2], total[2:3]
    count = float(frames * n)
    kurt_ref[...] = ((count + 1.0) / (count - 1.0)
                     * (count * second_moment / (mean_power * mean_power) - 1.0))
    own = jnp.zeros((1, part), jnp.float32)
    place = lax.broadcasted_iota(jnp.int32, (1, part), 1) + me * part
    for b in range(blocks):
        own = jnp.where(place // width == b, clean[b], own)
    spec_ref[...] = channels * own * mean_power / whole

    for slot, (first_row, count) in enumerate(pieces):
        def sent(off, carry, first_row=first_row, count=count, slot=slot):
            send(first_row, count, slot, off).wait_send()
            return carry

        lax.fori_loop(1, n, sent, 0)

    @pl.when(me < n - 1)
    def _():
        whole_halo().wait_send()

    out.wait()


def body(n, voltages, taps, flags):
    frames, channels = voltages.shape[1], voltages.shape[2]
    head = -(-(taps.shape[0] - 1) // ROWS) * ROWS
    outer = channels // LANES
    step = SUMMED * ROWS
    chunks = frames // step
    part = channels // n
    turn = 2.0 * np.pi * np.outer(np.arange(outer), np.arange(LANES)) / channels
    angle = 2.0 * np.pi * (np.outer(np.arange(LANES), np.arange(LANES)) % LANES) / LANES
    table = np.block([[np.cos(angle), -np.sin(angle)], [np.sin(angle), np.cos(angle)]]).astype(np.float32)
    table_high = table.astype(jnp.bfloat16)
    table_low = (table - table_high.astype(np.float32)).astype(jnp.bfloat16)
    vmem = pl.BlockSpec(memory_space=pltpu.VMEM)
    dynamic, kurtosis, spectrum = pl.pallas_call(
        functools.partial(kernel, n),
        out_shape=(
            jax.ShapeDtypeStruct((n, chunks * ROWS, part), jnp.float32),
            jax.ShapeDtypeStruct((1, part), jnp.float32),
            jax.ShapeDtypeStruct((1, part), jnp.float32),
        ),
        in_specs=[pl.BlockSpec(memory_space=pl.ANY)] * 5,
        out_specs=(pl.BlockSpec(memory_space=pl.ANY), vmem, vmem),
        scratch_shapes=[
            pltpu.VMEM(taps.shape, jnp.float32),
            pltpu.SMEM(flags.shape, jnp.int32),
            pltpu.VMEM((2, outer, LANES), jnp.float32),
            pltpu.VMEM((2, 2 * LANES, 2 * LANES), jnp.bfloat16),
            pltpu.SemaphoreType.DMA((4,)),
            pltpu.VMEM((2, outer, head + frames, LANES), jnp.float32),
            pltpu.VMEM((2, outer, step, LANES), jnp.float32),
            pltpu.VMEM((outer, step, 2 * LANES), jnp.float32),
            pltpu.VMEM((outer, ROWS, LANES), jnp.float32),
            pltpu.VMEM((outer, ROWS, LANES), jnp.float32),
            pltpu.VMEM((ROWS * outer, LANES), jnp.float32),
            pltpu.VMEM((ROWS * outer // LANES, LANES, LANES), jnp.float32),
            pltpu.VMEM((ROWS * outer, LANES), jnp.float32),
            pltpu.VMEM(((1 + chunks) * ROWS, channels), jnp.float32),
            pltpu.VMEM((n, (1 + chunks) * ROWS, part), jnp.float32),
            pltpu.SemaphoreType.DMA((chunks,)),
            pltpu.SemaphoreType.DMA,
            pltpu.SemaphoreType.DMA,
            pltpu.SemaphoreType.DMA((chunks, n)),
            pltpu.SemaphoreType.DMA((chunks, n)),
            pltpu.SemaphoreType.DMA,
        ],
        compiler_params=pltpu.CompilerParams(
            collective_id=0, has_side_effects=True, vmem_limit_bytes=65000 * 1024),
    )(voltages, taps, flags, jnp.asarray(np.stack([np.cos(turn), np.sin(turn)]), jnp.float32),
      jnp.asarray(np.stack([table_high, table_low])))
    return dynamic.reshape(n * chunks * ROWS, part), kurtosis.reshape(part), spectrum.reshape(part)


def solution(mesh):
    return jax.shard_map(
        functools.partial(body, mesh.shape["tm"]),
        mesh=mesh,
        in_specs=(P(None, ("stream", "tm"), None), P(), P("stream")),
        out_specs=(P("stream", "tm"), P(("stream", "tm")), P(("stream", "tm"))),
        check_vma=False,
    )
```

```python
import functools
import math

import jax
import jax.numpy as jnp
import numpy as np
from jax import lax
from jax.experimental import pallas as pl
from jax.experimental.pallas import tpu as pltpu
from jax.sharding import PartitionSpec as P

SUMMED = 4
LANES = 128
ROWS = 8


def rotate_by(value, k, n):
    re, im = value
    if k == 0:
        return re, im
    if 4 * k == n:
        return im, -re
    half = math.sqrt(0.5)
    if 8 * k == n:
        return (re + im) * half, (im - re) * half
    if 8 * k == 3 * n:
        return (im - re) * half, (re + im) * (-half)
    c = math.cos(2.0 * math.pi * k / n)
    s = math.sin(2.0 * math.pi * k / n)
    return re * c + im * s, im * c - re * s


def fft(values):
    n = len(values)
    if n == 1:
        return values
    even = fft(values[0::2])
    odd = fft(values[1::2])
    low, high = [], []
    for k in range(n // 2):
        tr, ti = rotate_by(odd[k], k, n)
        er, ei = even[k]
        low.append((er + tr, ei + ti))
        high.append((er - tr, ei - ti))
    return low + high


def kernel(n, x_hbm, taps_hbm, flags_hbm, turn_hbm, table_hbm,
           got_hbm,
           taps_ref, flags_ref, turn_ref, table_ref, side_sem, xbuf, ybuf, zbuf, m1buf, m2buf, pbuf, bbuf, tbuf, vbuf, sendbuf, recvbuf,
           load_sem, halo_send, halo_recv, send_sem, recv_sem, out_sem):
    me = lax.axis_index("tm")
    frames, channels = x_hbm.shape[1], x_hbm.shape[2]
    tap_count = taps_ref.shape[0]
    head = xbuf.shape[2] - frames
    outer = channels // LANES
    span = LANES // outer
    step = SUMMED * ROWS
    chunks = frames // step
    part = channels // n
    blocks = flags_ref.shape[0]
    width = channels // blocks

    def load(i, a):
        return pltpu.make_async_copy(
            x_hbm.at[:, pl.ds(i * step, step), pl.ds(pl.multiple_of(a * LANES, LANES), LANES)],
            xbuf.at[:, a, pl.ds(head + i * step, step), :], load_sem.at[i])

    def loaded(i):
        rows = xbuf.at[:, :, pl.ds(head + i * step, step), :]
        pltpu.make_async_copy(rows, rows, load_sem.at[i]).wait()

    sides = [pltpu.make_async_copy(source, target, side_sem.at[i]) for i, (source, target) in enumerate(
        ((taps_hbm, taps_ref), (flags_hbm, flags_ref), (turn_hbm, turn_ref), (table_hbm, table_ref)))]
    for side in sides:
        side.start()
    for i in range(chunks):
        def start_load(a, carry, i=i):
            load(i, a).start()
            return carry

        lax.fori_loop(0, outer, start_load, 0)

    barrier = pltpu.get_barrier_semaphore()

    def greet(off, carry):
        pl.semaphore_signal(barrier, inc=1, device_id={"tm": lax.rem(me + off, n)},
                            device_id_type=pl.DeviceIdType.MESH)
        return carry

    lax.fori_loop(1, n, greet, 0)
    pl.semaphore_wait(barrier, n - 1)

    def halo(a):
        return pltpu.make_async_remote_copy(
            src_ref=x_hbm.at[:, pl.ds(frames - head, head), pl.ds(pl.multiple_of(a * LANES, LANES), LANES)],
            dst_ref=xbuf.at[:, a, pl.ds(0, head), :],
            send_sem=halo_send, recv_sem=halo_recv,
            device_id={"tm": lax.rem(me + 1, n)}, device_id_type=pl.DeviceIdType.MESH)

    def whole_halo():
        return pltpu.make_async_remote_copy(
            src_ref=xbuf.at[:, :, pl.ds(0, head), :],
            dst_ref=xbuf.at[:, :, pl.ds(0, head), :],
            send_sem=halo_send, recv_sem=halo_recv,
            device_id={"tm": lax.rem(me + 1, n)}, device_id_type=pl.DeviceIdType.MESH)

    @pl.when(me < n - 1)
    def _():
        def start_halo(a, carry):
            halo(a).start()
            return carry

        lax.fori_loop(0, outer, start_halo, 0)

    @pl.when(me == 0)
    def _():
        xbuf[:, :, 0:head, :] = jnp.zeros((2, outer, head, LANES), jnp.float32)

    for side in sides:
        side.wait()
    m1buf[...] = jnp.zeros_like(m1buf)
    m2buf[...] = jnp.zeros_like(m2buf)
    lane = lax.broadcasted_iota(jnp.int32, (1, LANES), 1)
    clean = []
    clean_row = jnp.zeros((1, LANES), jnp.float32)
    for b in range(blocks):
        clean.append((1 - flags_ref[b]).astype(jnp.float32))
        clean_row = jnp.where(lane // (width // outer) == b, clean[b], clean_row)

    def relayout(count):
        for g in range(-(-count * outer // LANES)):
            tbuf[g] = bbuf[g * LANES:(g + 1) * LANES, :].T
        for r in range(count):
            g, place = (r * outer) // LANES, (r * outer) % LANES
            total = None
            for e1 in range(span):
                piece = tbuf[g, pl.ds(e1, outer, stride=span), :]
                shift = (e1 * outer - place) % LANES
                if shift:
                    piece = pltpu.roll(piece, shift, 1)
                total = piece if total is None else jnp.where(lane // outer == e1, piece, total)
            vbuf[r * outer:(r + 1) * outer, :] = total

    def send(first, count, slot, off):
        other = lax.rem(me + off, n)
        return pltpu.make_async_remote_copy(
            src_ref=sendbuf.at[pl.ds(first, count), pl.ds(pl.multiple_of(other * part, LANES), part)],
            dst_ref=recvbuf.at[me, pl.ds(first, count), :],
            send_sem=send_sem.at[slot, off], recv_sem=recv_sem.at[slot, me],
            device_id={"tm": other}, device_id_type=pl.DeviceIdType.MESH)

    def arrival(first, count, slot, source):
        return pltpu.make_async_remote_copy(
            src_ref=sendbuf.at[pl.ds(first, count), pl.ds(0, part)],
            dst_ref=recvbuf.at[source, pl.ds(first, count), :],
            send_sem=send_sem.at[slot, 0], recv_sem=recv_sem.at[slot, source],
            device_id={"tm": source}, device_id_type=pl.DeviceIdType.MESH)

    pieces = []
    order = list(range(1, chunks)) + [0]
    for slot, chunk in enumerate(order):
        if slot == 0:
            loaded(0)
        if chunk:
            loaded(chunk)
        else:
            @pl.when(me > 0)
            def _():
                whole_halo().wait_recv()
        base = head + chunk * step

        def fir(a, carry):
            columns = pl.ds(pl.multiple_of(a * LANES, LANES), LANES)
            coefficients = [jnp.broadcast_to(taps_ref[pl.ds(k, 1), columns], (ROWS, LANES))
                            for k in range(tap_count)]
            for s in range(2):
                sums = [None] * SUMMED
                for o in range(1 - tap_count, (SUMMED - 1) * ROWS + 1):
                    value = xbuf[s, a, pl.ds(base + o, ROWS), :]
                    for j in range(SUMMED):
                        if 0 <= j * ROWS - o < tap_count:
                            term = coefficients[j * ROWS - o] * value
                            sums[j] = term if sums[j] is None else sums[j] + term
                for j in range(SUMMED):
                    ybuf[s, a, j * ROWS:(j + 1) * ROWS, :] = sums[j]
            return carry

        lax.fori_loop(0, outer, fir, 0, unroll=2)

        def columns_fft(j, carry):
            rows = pl.ds(pl.multiple_of(j * ROWS, ROWS), ROWS)
            result = fft([(ybuf[0, a, rows, :], ybuf[1, a, rows, :]) for a in range(outer)])
            for d in range(outer):
                re, im = result[d]
                c, s = turn_ref[0, d:d + 1, :], turn_ref[1, d:d + 1, :]
                zbuf[d, rows, 0:LANES] = re * c + im * s
                zbuf[d, rows, LANES:2 * LANES] = im * c - re * s
            return carry

        lax.fori_loop(0, SUMMED, columns_fft, 0)

        group = 8

        def lanes_dft(g, row_sum):
            z = zbuf[pl.ds(g * group, group), :, :].reshape(group * step, 2 * LANES)
            high = z.astype(jnp.bfloat16)
            low = (z - high.astype(jnp.float32)).astype(jnp.bfloat16)
            y = (jnp.dot(high, table_ref[0], preferred_element_type=jnp.float32)
                 + jnp.dot(low, table_ref[0], preferred_element_type=jnp.float32)
                 + jnp.dot(high, table_ref[1], preferred_element_type=jnp.float32))
            re, im = y[:, :LANES], y[:, LANES:]
            power = re * re + im * im
            pbuf[...] = power
            for k in range(group):
                piece = [pbuf[pl.ds(k * step + j, ROWS, stride=SUMMED), :] for j in range(SUMMED)]
                first = (piece[0] + piece[1]) + (piece[2] + piece[3])
                second = ((piece[0] * piece[0] + piece[1] * piece[1])
                          + (piece[2] * piece[2] + piece[3] * piece[3]))
                d = g * group + k
                bbuf[pl.ds(d, ROWS, stride=outer), :] = first
                m1buf[d] = m1buf[d] + first
                m2buf[d] = m2buf[d] + second
                row_sum = row_sum + first
            return row_sum

        row_sum = lax.fori_loop(0, outer // group, lanes_dft, jnp.zeros((ROWS, LANES), jnp.float32))
        row_total = jnp.sum(row_sum * clean_row, axis=1, keepdims=True)
        scale = channels / row_total
        relayout(ROWS)
        first_row = ROWS * (1 + chunk)
        for q in range(outer):
            tile = vbuf[pl.ds(q, ROWS, stride=outer), :]
            sendbuf[first_row:first_row + ROWS, q * LANES:(q + 1) * LANES] = (
                tile * (scale * clean[q * LANES // width]))
        count = ROWS
        if slot == chunks - 1:
            first = jnp.sum(m1buf[...], axis=1)
            second = jnp.sum(m2buf[...], axis=1)
            bbuf[0:outer, :] = first
            bbuf[outer:2 * outer, :] = second
            bbuf[2 * outer:, :] = jnp.zeros((bbuf.shape[0] - 2 * outer, LANES), jnp.float32)
            relayout(2)
            group_sum = jnp.sum(jnp.sum(first, axis=0, keepdims=True) * clean_row, axis=1, keepdims=True)
            vbuf[2 * outer:3 * outer, :] = jnp.broadcast_to(group_sum, (outer, LANES))
            for q in range(outer):
                sendbuf[0:ROWS, q * LANES:(q + 1) * LANES] = vbuf[pl.ds(q, ROWS, stride=outer), :]
            first_row, count = 0, 2 * ROWS
        pieces.append((first_row, count))

        def start(off, carry, first_row=first_row, count=count, slot=slot):
            send(first_row, count, slot, off).start()
            return carry

        lax.fori_loop(1, n, start, 0)
        recvbuf[me, first_row:first_row + count, :] = sendbuf[
            first_row:first_row + count, pl.ds(pl.multiple_of(me * part, LANES), part)]

    for slot, (first_row, count) in enumerate(pieces):
        def receive(off, carry, first_row=first_row, count=count, slot=slot):
            arrival(first_row, count, slot, lax.rem(me + n - off, n)).wait_recv()
            return carry

        lax.fori_loop(1, n, receive, 0)

    out = pltpu.make_async_copy(recvbuf, got_hbm, out_sem)
    out.start()

    for slot, (first_row, count) in enumerate(pieces):
        def sent(off, carry, first_row=first_row, count=count, slot=slot):
            send(first_row, count, slot, off).wait_send()
            return carry

        lax.fori_loop(1, n, sent, 0)

    @pl.when(me < n - 1)
    def _():
        whole_halo().wait_send()

    out.wait()


def finish(n, got_hbm, flags_hbm, dyn_hbm, kurt_hbm, spec_hbm, got, flags_ref, result, sem):
    moments = pltpu.make_async_copy(got_hbm.at[:, pl.ds(0, ROWS), :], got.at[:, pl.ds(0, ROWS), :], sem.at[0])
    rows = pltpu.make_async_copy(
        got_hbm.at[:, pl.ds(ROWS, got.shape[1] - ROWS), :], got.at[:, pl.ds(ROWS, got.shape[1] - ROWS), :], sem.at[1])
    side = pltpu.make_async_copy(flags_hbm, flags_ref, sem.at[2])
    moments.start()
    side.start()
    rows.start()
    moments.wait()
    side.wait()
    part = got.shape[2]
    channels = part * n
    blocks = flags_ref.shape[0]
    width = channels // blocks
    total = got[0, 0:ROWS, :]
    for source in range(1, n):
        total = total + got[source, 0:ROWS, :]
    mean_power, second_moment, whole = total[0:1], total[1:2], total[2:3]
    count = float((got.shape[1] - ROWS) * SUMMED * n)
    own = jnp.zeros((1, part), jnp.float32)
    place = lax.broadcasted_iota(jnp.int32, (1, part), 1) + lax.axis_index("tm") * part
    for b in range(blocks):
        own = jnp.where(place // width == b, (1 - flags_ref[b]).astype(jnp.float32), own)
    result[0] = ((count + 1.0) / (count - 1.0)
                 * (count * second_moment / (mean_power * mean_power) - 1.0))
    result[1] = channels * own * mean_power / whole
    kurt = pltpu.make_async_copy(result.at[0], kurt_hbm, sem.at[0])
    spec = pltpu.make_async_copy(result.at[1], spec_hbm, sem.at[2])
    kurt.start()
    spec.start()
    rows.wait()
    dyn = pltpu.make_async_copy(got.at[:, pl.ds(ROWS, got.shape[1] - ROWS), :], dyn_hbm, sem.at[1])
    dyn.start()
    kurt.wait()
    spec.wait()
    dyn.wait()


def body(n, voltages, taps, flags):
    frames, channels = voltages.shape[1], voltages.shape[2]
    head = -(-(taps.shape[0] - 1) // ROWS) * ROWS
    outer = channels // LANES
    step = SUMMED * ROWS
    chunks = frames // step
    part = channels // n
    turn = 2.0 * np.pi * np.outer(np.arange(outer), np.arange(LANES)) / channels
    angle = 2.0 * np.pi * (np.outer(np.arange(LANES), np.arange(LANES)) % LANES) / LANES
    table = np.block([[np.cos(angle), -np.sin(angle)], [np.sin(angle), np.cos(angle)]]).astype(np.float32)
    table_high = table.astype(jnp.bfloat16)
    table_low = (table - table_high.astype(np.float32)).astype(jnp.bfloat16)
    got = pl.pallas_call(
        functools.partial(kernel, n),
        out_shape=jax.ShapeDtypeStruct((n, (1 + chunks) * ROWS, part), jnp.float32),
        in_specs=[pl.BlockSpec(memory_space=pl.ANY)] * 5,
        out_specs=pl.BlockSpec(memory_space=pl.ANY),
        scratch_shapes=[
            pltpu.VMEM(taps.shape, jnp.float32),
            pltpu.SMEM(flags.shape, jnp.int32),
            pltpu.VMEM((2, outer, LANES), jnp.float32),
            pltpu.VMEM((2, 2 * LANES, 2 * LANES), jnp.bfloat16),
            pltpu.SemaphoreType.DMA((4,)),
            pltpu.VMEM((2, outer, head + frames, LANES), jnp.float32),
            pltpu.VMEM((2, outer, step, LANES), jnp.float32),
            pltpu.VMEM((outer, step, 2 * LANES), jnp.float32),
            pltpu.VMEM((outer, ROWS, LANES), jnp.float32),
            pltpu.VMEM((outer, ROWS, LANES), jnp.float32),
            pltpu.VMEM((8 * step, LANES), jnp.float32),
            pltpu.VMEM((ROWS * outer, LANES), jnp.float32),
            pltpu.VMEM((ROWS * outer // LANES, LANES, LANES), jnp.float32),
            pltpu.VMEM((ROWS * outer, LANES), jnp.float32),
            pltpu.VMEM(((1 + chunks) * ROWS, channels), jnp.float32),
            pltpu.VMEM((n, (1 + chunks) * ROWS, part), jnp.float32),
            pltpu.SemaphoreType.DMA((chunks,)),
            pltpu.SemaphoreType.DMA,
            pltpu.SemaphoreType.DMA,
            pltpu.SemaphoreType.DMA((chunks, n)),
            pltpu.SemaphoreType.DMA((chunks, n)),
            pltpu.SemaphoreType.DMA,
        ],
        compiler_params=pltpu.CompilerParams(
            collective_id=0, has_side_effects=True, vmem_limit_bytes=65000 * 1024),
    )(voltages, taps, flags, jnp.asarray(np.stack([np.cos(turn), np.sin(turn)]), jnp.float32),
      jnp.asarray(np.stack([table_high, table_low])))
    dynamic, kurtosis, spectrum = pl.pallas_call(
        functools.partial(finish, n),
        out_shape=(
            jax.ShapeDtypeStruct((n, chunks * ROWS, part), jnp.float32),
            jax.ShapeDtypeStruct((1, part), jnp.float32),
            jax.ShapeDtypeStruct((1, part), jnp.float32),
        ),
        in_specs=[pl.BlockSpec(memory_space=pl.ANY)] * 2,
        out_specs=[pl.BlockSpec(memory_space=pl.ANY)] * 3,
        scratch_shapes=[
            pltpu.VMEM((n, (1 + chunks) * ROWS, part), jnp.float32),
            pltpu.SMEM(flags.shape, jnp.int32),
            pltpu.VMEM((2, 1, part), jnp.float32),
            pltpu.SemaphoreType.DMA((3,)),
        ],
        compiler_params=pltpu.CompilerParams(vmem_limit_bytes=65000 * 1024),
    )(got, flags)
    return dynamic.reshape(n * chunks * ROWS, part), kurtosis.reshape(part), spectrum.reshape(part)


def solution(mesh):
    return jax.shard_map(
        functools.partial(body, mesh.shape["tm"]),
        mesh=mesh,
        in_specs=(P(None, ("stream", "tm"), None), P(), P("stream")),
        out_specs=(P("stream", "tm"), P(("stream", "tm")), P(("stream", "tm"))),
        check_vma=False,
    )
```
